256 devices in a mesh: dp: 64 (over z, x, core), rep: 4 (over y).
Axes of the slice: x: 4, y: 4, z: 8, core: 2. Of those that a mesh axis runs over, the one named last changes fastest.
Arguments:
- tokens: bfloat16 [65536, 2048], P(('rep', 'dp')), parts along dimension 0, may hold values from -12 to 12
- router: bfloat16 [8192, 64], P('rep'), parts along dimension 0, may hold values from -12 to 12
- w_gate: bfloat16 [64, 2048, 768], P('dp'), may hold values from -0.125 to 0.125
- w_up: bfloat16 [64, 2048, 768], P('dp'), may hold values from -0.125 to 0.125
- w_down: bfloat16 [64, 768, 2048], P('dp'), may hold values from -0.21875 to 0.21875
- picks: int32 [256, 256], P(('rep', 'dp')), parts along dimension 0, may hold values from 0 to 16383, as said below
Outputs:
- combined: bfloat16 [65536, 2048], P(('rep', 'dp')), parts along dimension 0
The draws below stay inside these ranges and needn't reach their ends.
There are 4 independent parts, one for each index of `rep`. The reference program is written for one: setup_inputs(seed, part) draws one part's arguments, and reference() takes and returns one part's arrays. A program takes and returns all parts, laid end to end along the dimension named above; an argument that names none is the same for every part. Nothing has to cross between parts.
Inputs may be any that keep to these rules, and one draw needn't show every extreme that they name: `picks`: row e holds 256 different tokens taken by expert e, sorted by the device that holds them (256 tokens each, in order); at most 6 of them lie among one device's tokens, and in every row exactly 6 lie among some device's tokens.
All inputs are finite; a program needn't handle non-finite values.
Results may differ from the reference program's by a relative error of at most 0.0062.
Values may be sent and summed in bfloat16 or wider, within the bound.
A program may use at most 64 MiB of HBM per device.

```python
import math
import jax
import jax.numpy as jnp
from jax import lax

D = 2048
FF = 768
TOK_DEV = 256
BASE = 4
EXPERTS = 64
CAP = 256
TOKENS = 16384


def draw_router(key, part):
    base = jax.random.normal(jax.random.fold_in(key, 21), (D, EXPERTS), jnp.float32)
    matrix = base * (1.0 / math.sqrt(D))
    return jnp.clip(matrix, -12.0, 12.0).astype(jnp.bfloat16)


def draw_tokens(key, part):
    values = jax.random.normal(jax.random.fold_in(key, 31), (TOKENS, D), jnp.float32)
    return jnp.clip(values, -12.0, 12.0).astype(jnp.bfloat16)


def draw_picks(key, part):
    key_pair, key_shift, key_order = jax.random.split(key, 3)
    half_base = BASE // 2
    pairing = jax.vmap(lambda subkey: jax.random.permutation(subkey, EXPERTS))(jax.random.split(key_pair, EXPERTS))
    offsets = jax.random.randint(key_shift, (EXPERTS, EXPERTS // 2), -half_base, half_base + 1)
    offsets = offsets.at[:, 0].set(half_base)
    paired = (jnp.concatenate([offsets, -offsets], axis=1) + BASE).astype(jnp.int32)
    rows_at = jnp.arange(EXPERTS, dtype=jnp.int32)[:, None]
    counts = jnp.zeros((EXPERTS, EXPERTS), jnp.int32).at[rows_at, pairing].set(paired)
    block_end = jnp.cumsum(counts, axis=1)
    starts = block_end - counts
    slot_pos = jnp.arange(CAP, dtype=jnp.int32)
    source_of = jnp.sum((slot_pos[None, :, None] >= block_end[:, None, :]).astype(jnp.int32), axis=2)
    within = slot_pos[None, :] - jnp.take_along_axis(starts, source_of, axis=1)
    scores = jax.random.randint(key_order, (EXPERTS, EXPERTS, TOK_DEV), 0, 1 << 30)
    shuffled = jnp.argsort(scores, axis=2, stable=True).astype(jnp.int32)
    shuffled_rows = shuffled.reshape(EXPERTS * EXPERTS, TOK_DEV)
    row_index = rows_at * EXPERTS + source_of
    local_pick = shuffled_rows[row_index, within]
    return (source_of * TOK_DEV + local_pick).astype(jnp.int32)


def steps_of(key, dims, shards, smallest, largest):
    level = 1.0
    for dim, blocks in shards:
        steps = jax.random.uniform(jax.random.fold_in(jax.random.fold_in(key, 6), dim), (blocks,), jnp.float32, smallest / len(shards), largest / len(shards))
        level = level * jnp.repeat(jnp.exp(steps), dims[dim] // blocks).reshape((-1,) + (1,) * (len(dims) - 1 - dim))
    return level


def scatter_about(own_key, shape, deviation, reach, cuts=(), kind=jnp.bfloat16):
    array = jax.random.normal(own_key, shape, jnp.float32) * deviation
    if len(cuts) > 0:
        array = steps_of(own_key, shape, cuts, -0.22, 0.18) * array
    return jnp.clip(array, min=-reach, max=reach).astype(kind)


def setup_inputs(seed: int = 0, part: int = 0) -> dict:
    arg_keys = jax.random.split(jax.random.key(seed), 7)
    own_keys = jax.random.split(jax.random.fold_in(arg_keys[6], part), 7)
    return {
        "tokens": draw_tokens(jax.random.fold_in(jax.random.fold_in(arg_keys[6], part), 71), part),
        "router": draw_router(jax.random.fold_in(jax.random.fold_in(arg_keys[6], part), 71), part),
        "w_gate": scatter_about(arg_keys[2], (EXPERTS, D, FF), D ** -0.5, 0.125, ((0, 64),)),
        "w_up": scatter_about(arg_keys[3], (EXPERTS, D, FF), D ** -0.5, 0.125, ((0, 64),)),
        "w_down": scatter_about(arg_keys[4], (EXPERTS, FF, D), FF ** -0.5, 0.21875, ((0, 64),)),
        "picks": draw_picks(jax.random.fold_in(jax.random.fold_in(arg_keys[6], part), 71), part),
    }


def reference(tokens, router, w_gate, w_up, w_down, picks):
    logits = jnp.dot(tokens, router, preferred_element_type=jnp.float32)
    shares = jax.nn.softmax(logits, axis=1)
    gates = (EXPERTS * jnp.take_along_axis(shares.T, picks, axis=1)).astype(jnp.bfloat16)

    def one_expert(inputs):
        gate_w, up_w, down_w, chosen_index, gate_row = inputs
        chosen = tokens[chosen_index]
        gate_act = jnp.dot(chosen, gate_w, preferred_element_type=jnp.float32)
        up_act = jnp.dot(chosen, up_w, preferred_element_type=jnp.float32)
        hidden = (gate_row.astype(jnp.float32)[:, None] * jax.nn.silu(gate_act) * up_act).astype(jnp.bfloat16)
        return jnp.dot(hidden, down_w, preferred_element_type=jnp.float32).astype(jnp.bfloat16)

    results = lax.map(one_expert, (w_gate, w_up, w_down, picks, gates))
    width = tokens.shape[1]
    combined = jnp.zeros((tokens.shape[0], width), jnp.float32).at[picks.reshape(-1)].add(
        results.reshape(-1, width).astype(jnp.float32))
    return combined.astype(jnp.bfloat16)
```

```python
import functools

import jax
import jax.numpy as jnp
from jax import lax
from jax.experimental import pallas as pl
from jax.experimental.pallas import tpu as pltpu
from jax.sharding import PartitionSpec as P

MOST = 6
PLANE = 8
SUB, LANE = 16, 128
MESH = pl.DeviceIdType.MESH


def swap_matrix():
    row = lax.broadcasted_iota(jnp.int32, (SUB * SUB, SUB * SUB), 0)
    col = lax.broadcasted_iota(jnp.int32, (SUB * SUB, SUB * SUB), 1)
    swapped = (col % SUB) * SUB + col // SUB
    return (row == swapped).astype(jnp.float32).astype(jnp.bfloat16)


def swap(matrix, stacked):
    return jnp.dot(matrix, stacked, preferred_element_type=jnp.float32).astype(jnp.bfloat16)


def plane_tiles(buffer, plane, part):
    tiles = [
        buffer[plane * PLANE + member, 2 * part + half]
        for half in range(2)
        for member in range(PLANE)
    ]
    return jnp.concatenate(tiles, axis=0)


def to_rows(matrix, buffer, planes, target, target_row):
    jobs = [(plane, part) for plane in planes for part in range(MOST // 2)]
    for first in range(0, len(jobs), 2):
        pair = jobs[first : first + 2]
        stacked = jnp.concatenate([plane_tiles(buffer, *job) for job in pair], axis=1)
        moved = swap(matrix, stacked)
        for which in range(len(pair)):
            at = target_row + (first + which) * SUB
            for chunk in range(SUB):
                target[pl.ds(at, SUB), chunk * LANE : (chunk + 1) * LANE] = moved[
                    chunk * SUB : (chunk + 1) * SUB, which * LANE : (which + 1) * LANE
                ]


def to_tiles(matrix, rows, first_row):
    def stack(at):
        return jnp.concatenate(
            [rows[pl.ds(at, SUB), chunk * LANE : (chunk + 1) * LANE] for chunk in range(SUB)],
            axis=0,
        )

    stacked = jnp.concatenate([stack(first_row), stack(first_row + SUB)], axis=1)
    moved = swap(matrix, stacked)
    return [
        moved[row * SUB : (row + 1) * SUB, half * LANE : (half + 1) * LANE]
        for half in range(2)
        for row in range(SUB)
    ]


def kernel(
    n,
    tokens_hbm,
    router_hbm,
    gate_hbm,
    up_hbm,
    down_hbm,
    picks_ref,
    out_ref,
    tokens,
    router,
    gate_w,
    up_w,
    down_w,
    token_tiles,
    gates_t,
    all_picks,
    slots_v,
    slots_s,
    mix_t,
    mix,
    send_buf,
    recv_buf,
    rows,
    hidden,
    result_rows,
    result_buf,
    return_buf,
    return_rows,
    load_sem,
    slot_sem,
    local_sem,
    pick_send,
    pick_recv,
    row_send,
    row_recv,
    result_send,
    result_recv,
):
    me = lax.axis_index("dp")
    planes = n // PLANE
    my_plane = me // PLANE
    tok_dev, width = tokens.shape
    capacity = picks_ref.shape[1]
    steps = planes // 2

    def step_planes(step):
        up = step + 1
        down = jnp.where(step == steps - 1, 0, planes - 1 - step)
        return lax.rem(my_plane + up, planes), lax.rem(my_plane + down, planes)

    loads = [
        pltpu.make_async_copy(tokens_hbm, tokens, load_sem.at[0]),
        pltpu.make_async_copy(router_hbm, router, load_sem.at[1]),
        pltpu.make_async_copy(gate_hbm.at[0], gate_w, load_sem.at[2]),
        pltpu.make_async_copy(up_hbm.at[0], up_w, load_sem.at[3]),
        pltpu.make_async_copy(down_hbm.at[0], down_w, load_sem.at[4]),
    ]
    for load in loads:
        load.start()

    barrier = pltpu.get_barrier_semaphore()

    @pl.loop(1, n)
    def _(shift):
        pl.semaphore_signal(
            barrier, inc=1, device_id={"dp": lax.rem(me + shift, n)}, device_id_type=MESH
        )

    pl.semaphore_wait(barrier, n - 1)

    def pick_copy(target):
        return pltpu.make_async_remote_copy(
            src_ref=picks_ref,
            dst_ref=all_picks.at[me],
            send_sem=pick_send,
            recv_sem=pick_recv.at[my_plane],
            device_id={"dp": target},
            device_id_type=MESH,
        )

    @pl.loop(0, steps)
    def _(step):
        for plane in step_planes(step):

            @pl.loop(0, PLANE)
            def _(member):
                target = plane * PLANE + member

                @pl.when(target != me)
                def _():
                    pick_copy(target).start()

    all_picks[me] = picks_ref[...]

    matrix = swap_matrix()
    loads[0].wait()
    loads[1].wait()
    logits = jnp.dot(tokens[...], router[...], preferred_element_type=jnp.float32)
    logits = logits.T
    powers = jnp.exp(logits - jnp.max(logits, axis=0, keepdims=True))
    shares = powers / jnp.sum(powers, axis=0, keepdims=True)
    gates_t[...] = (n * shares).astype(jnp.bfloat16).astype(jnp.float32)

    @pl.loop(0, tok_dev // (2 * SUB))
    def _(block):
        at = pl.multiple_of(block * 2 * SUB, 2 * SUB)
        tiles = to_tiles(matrix, tokens, at)
        for index, tile in enumerate(tiles):
            token_tiles[at + index] = tile

    token_tiles[tok_dev] = jnp.zeros((SUB, LANE), jnp.bfloat16)

    def row_copy(target):
        return pltpu.make_async_remote_copy(
            src_ref=send_buf.at[target],
            dst_ref=recv_buf.at[me],
            send_sem=row_send,
            recv_sem=row_recv.at[my_plane],
            device_id={"dp": target},
            device_id_type=MESH,
        )

    def result_copy(target):
        return pltpu.make_async_remote_copy(
            src_ref=result_buf.at[target],
            dst_ref=return_buf.at[me],
            send_sem=result_send,
            recv_sem=result_recv.at[my_plane],
            device_id={"dp": target},
            device_id_type=MESH,
        )

    own_rows = pltpu.make_async_copy(send_buf.at[me], recv_buf.at[me], local_sem.at[0])
    own_results = pltpu.make_async_copy(result_buf.at[me], return_buf.at[me], local_sem.at[1])

    def send_plane(plane, copy, own):
        @pl.loop(0, PLANE)
        def _(member):
            target = plane * PLANE + member

            @pl.when(target != me)
            def _():
                copy(target).start()

            @pl.when(target == me)
            def _():
                own.start()

    def wait_plane(plane, buffer, semaphores, own):
        @pl.when(plane != my_plane)
        def _():
            part = buffer.at[pl.ds(plane * PLANE, PLANE)]
            pltpu.make_async_copy(part, part, semaphores.at[plane]).wait()

        @pl.when(plane == my_plane)
        def _():
            part = buffer.at[pl.ds(plane * PLANE, PLANE - 1)]
            pltpu.make_async_copy(part, part, semaphores.at[plane]).wait()
            if own is not None:
                own.wait()

    lane = lax.broadcasted_iota(jnp.int32, (PLANE, capacity), 1)
    token_lane = lax.broadcasted_iota(jnp.int32, (PLANE, tok_dev), 1)
    slot_lane = lax.broadcasted_iota(jnp.int32, (PLANE, LANE), 1)

    @pl.loop(0, steps)
    def _(step):
        for plane in step_planes(step):
            wait_plane(plane, all_picks, pick_recv, None)
            first = pl.multiple_of(plane * PLANE, PLANE)
            picked = all_picks[pl.ds(first, PLANE)].reshape(PLANE, capacity)
            local = picked - me * tok_dev
            mine = (local >= 0) & (local < tok_dev)
            before = jnp.sum((local < 0).astype(jnp.int32), axis=1, keepdims=True)
            place = lane - before
            label = jnp.where(mine, local + 1, 0)
            gates = gates_t[pl.ds(first, PLANE), :]
            table = jnp.full((PLANE, LANE), tok_dev, jnp.int32)
            for slot in range(MOST):
                found = jnp.sum(jnp.where(place == slot, label, 0), axis=1, keepdims=True)
                token = found - 1
                mix_t[pl.ds(pl.multiple_of(plane * PLANE * MOST, PLANE) + slot * PLANE, PLANE), :] = (
                    jnp.where(token_lane == token, gates, 0.0)
                )
                token = jnp.where(found > 0, token, tok_dev)
                table = jnp.where(slot_lane == slot, token, table)
            slots_v[plane] = table
            pltpu.make_async_copy(slots_v.at[plane], slots_s.at[plane], slot_sem).start()
            pltpu.make_async_copy(slots_v.at[plane], slots_s.at[plane], slot_sem).wait()
            for member in range(PLANE):
                for slot in range(MOST):
                    token = jnp.clip(slots_s[plane, member, slot], 0, tok_dev)
                    send_buf[plane * PLANE + member, slot] = token_tiles[token]
            send_plane(plane, row_copy, own_rows)

    mix[...] = mix_t[...].T.astype(jnp.bfloat16)

    for load in loads[2:]:
        load.wait()

    half = PLANE * MOST

    @pl.loop(0, steps)
    def _(step):
        pair = step_planes(step)
        for plane in pair:
            wait_plane(plane, recv_buf, row_recv, own_rows)
        to_rows(matrix, recv_buf, pair, rows, 0)
        taken = rows[...]
        block = 256
        for at in range(0, gate_w.shape[1], block):
            gate_act = jnp.dot(taken, gate_w[:, at : at + block], preferred_element_type=jnp.float32)
            up_act = jnp.dot(taken, up_w[:, at : at + block], preferred_element_type=jnp.float32)
            hidden[:, at : at + block] = (
                gate_act / (1.0 + jnp.exp(-gate_act)) * up_act
            ).astype(jnp.bfloat16)
        held = hidden[...]
        for at in range(0, width, block):
            result_rows[:, at : at + block] = jnp.dot(
                held, down_w[:, at : at + block], preferred_element_type=jnp.float32
            ).astype(jnp.bfloat16)
        for pack in range(2 * half // (2 * SUB)):
            tiles = to_tiles(matrix, result_rows, pack * 2 * SUB)
            for index, tile in enumerate(tiles):
                row = pack * 2 * SUB + index
                plane = pair[row // half]
                slot, member = divmod(row % half, PLANE)
                result_buf[plane * PLANE + member, slot] = tile
        for plane in pair:
            send_plane(plane, result_copy, own_results)

    @pl.loop(0, steps)
    def _(step):
        for plane in step_planes(step):
            wait_plane(plane, return_buf, result_recv, own_results)
            to_rows(
                matrix, return_buf, (plane,), return_rows, pl.multiple_of(plane * half, SUB)
            )

    weights = mix[...]
    for at in range(0, width, 256):
        out_ref[:, at : at + 256] = jnp.dot(
            weights, return_rows[:, at : at + 256], preferred_element_type=jnp.float32
        ).astype(jnp.bfloat16)

    def drain(buffer, semaphore):
        part = buffer.at[pl.ds(0, n - 1)]
        pltpu.make_async_copy(part, part, semaphore).wait()

    drain(all_picks, pick_send)
    drain(send_buf, row_send)
    drain(result_buf, result_send)


def layer(n, tokens, router, w_gate, w_up, w_down, picks):
    tok_dev, width = tokens.shape
    hidden_width = w_gate.shape[2]
    capacity = picks.shape[1]
    planes = n // PLANE
    vmem = pl.BlockSpec(memory_space=pltpu.VMEM)
    anywhere = pl.BlockSpec(memory_space=pl.ANY)
    block = (n, MOST, SUB, LANE)
    bf16 = jnp.bfloat16
    group = 2 * PLANE * MOST
    return pl.pallas_call(
        functools.partial(kernel, n),
        out_shape=jax.ShapeDtypeStruct((tok_dev, width), bf16),
        in_specs=[anywhere] * 5 + [vmem],
        out_specs=vmem,
        scratch_shapes=[
            pltpu.VMEM((tok_dev, width), bf16),
            pltpu.VMEM(router.shape, bf16),
            pltpu.VMEM((width, hidden_width), bf16),
            pltpu.VMEM((width, hidden_width), bf16),
            pltpu.VMEM((hidden_width, width), bf16),
            pltpu.VMEM((tok_dev + 1, SUB, LANE), bf16),
            pltpu.VMEM((n, tok_dev), jnp.float32),
            pltpu.VMEM((n, 1, capacity), jnp.int32),
            pltpu.VMEM((planes, PLANE, LANE), jnp.int32),
            pltpu.SMEM((planes, PLANE, LANE), jnp.int32),
            pltpu.VMEM((n * MOST, tok_dev), jnp.float32),
            pltpu.VMEM((tok_dev, n * MOST), bf16),
            pltpu.VMEM(block, bf16),
            pltpu.VMEM(block, bf16),
            pltpu.VMEM((group, width), bf16),
            pltpu.VMEM((group, hidden_width), bf16),
            pltpu.VMEM((group, width), bf16),
            pltpu.VMEM(block, bf16),
            pltpu.VMEM(block, bf16),
            pltpu.VMEM((n * MOST, width), bf16),
            pltpu.SemaphoreType.DMA((5,)),
            pltpu.SemaphoreType.DMA,
            pltpu.SemaphoreType.DMA((2,)),
            pltpu.SemaphoreType.DMA,
            pltpu.SemaphoreType.DMA((planes,)),
            pltpu.SemaphoreType.DMA,
            pltpu.SemaphoreType.DMA((planes,)),
            pltpu.SemaphoreType.DMA,
            pltpu.SemaphoreType.DMA((planes,)),
        ],
        compiler_params=pltpu.CompilerParams(collective_id=0, has_side_effects=True),
    )(tokens, router, w_gate, w_up, w_down, picks)


def solution(mesh):
    n = mesh.shape["dp"]
    return jax.shard_map(
        functools.partial(layer, n),
        mesh=mesh,
        in_specs=(
            P(("rep", "dp"), None),
            P("rep", None),
            P("dp", None, None),
            P("dp", None, None),
            P("dp", None, None),
            P(("rep", "dp"), None),
        ),
        out_specs=P(("rep", "dp"), None),
        check_vma=False,
    )
```

```python
import functools

import jax
import jax.numpy as jnp
from jax import lax
from jax.experimental import pallas as pl
from jax.experimental.pallas import tpu as pltpu
from jax.sharding import PartitionSpec as P

MOST = 6
PLANE = 8
SUB, LANE = 16, 128
MESH = pl.DeviceIdType.MESH
GOING = ((1, 7), (2, 6), (3, 5), (4, 0))
COMING = ((1, 7), (2, 6), (3, 5), (4, 0))


def swap_matrix():
    row = lax.broadcasted_iota(jnp.int32, (SUB * SUB, SUB * SUB), 0)
    col = lax.broadcasted_iota(jnp.int32, (SUB * SUB, SUB * SUB), 1)
    swapped = (col % SUB) * SUB + col // SUB
    return (row == swapped).astype(jnp.float32).astype(jnp.bfloat16)


def swap(matrix, stacked):
    return jnp.dot(matrix, stacked, preferred_element_type=jnp.float32).astype(jnp.bfloat16)


def plane_tiles(buffer, plane, part):
    tiles = [
        buffer[plane * PLANE + member, 2 * part + half]
        for half in range(2)
        for member in range(PLANE)
    ]
    return jnp.concatenate(tiles, axis=0)


def to_rows(matrix, buffer, planes, target, target_row):
    jobs = [(plane, part) for plane in planes for part in range(MOST // 2)]
    for first in range(0, len(jobs), 2):
        pair = jobs[first : first + 2]
        stacked = jnp.concatenate([plane_tiles(buffer, *job) for job in pair], axis=1)
        moved = swap(matrix, stacked)
        for which in range(len(pair)):
            at = target_row + (first + which) * SUB
            for chunk in range(SUB):
                target[pl.ds(at, SUB), chunk * LANE : (chunk + 1) * LANE] = moved[
                    chunk * SUB : (chunk + 1) * SUB, which * LANE : (which + 1) * LANE
                ]


def to_tiles(matrix, rows, first_row):
    def stack(at):
        return jnp.concatenate(
            [rows[pl.ds(at, SUB), chunk * LANE : (chunk + 1) * LANE] for chunk in range(SUB)],
            axis=0,
        )

    stacked = jnp.concatenate([stack(first_row), stack(first_row + SUB)], axis=1)
    moved = swap(matrix, stacked)
    return [
        moved[row * SUB : (row + 1) * SUB, half * LANE : (half + 1) * LANE]
        for half in range(2)
        for row in range(SUB)
    ]


def kernel(
    n,
    tokens_hbm,
    router_hbm,
    gate_hbm,
    up_hbm,
    down_hbm,
    picks_hbm,
    out_ref,
    tokens,
    router,
    gate_w,
    up_w,
    down_w,
    token_tiles,
    gates_t,
    all_picks,
    slots_v,
    slots_s,
    mix_t,
    mix,
    send_buf,
    recv_buf,
    rows,
    hidden,
    result_rows,
    result_buf,
    return_buf,
    return_rows,
    load_sem,
    slot_sem,
    local_sem,
    pick_send,
    pick_recv,
    row_send,
    row_recv,
    result_send,
    result_recv,
):
    me = lax.axis_index("dp")
    planes = n // PLANE
    my_plane = me // PLANE
    tok_dev, width = tokens.shape
    capacity = picks_hbm.shape[1]
    steps = planes // 2
    half = PLANE * MOST

    def step_planes(order, step):
        pair = order[-1]
        for index in range(steps - 1):
            pair = [jnp.where(step == index, *both) for both in zip(order[index], pair)]
        return [lax.rem(my_plane + distance, planes) for distance in pair]

    loads = [
        pltpu.make_async_copy(tokens_hbm, tokens, load_sem.at[0]),
        pltpu.make_async_copy(router_hbm, router, load_sem.at[1]),
        pltpu.make_async_copy(gate_hbm.at[0], gate_w, load_sem.at[2]),
        pltpu.make_async_copy(up_hbm.at[0], up_w, load_sem.at[3]),
        pltpu.make_async_copy(down_hbm.at[0], down_w, load_sem.at[4]),
    ]
    own_picks = pltpu.make_async_copy(picks_hbm, all_picks.at[me], local_sem.at[2])
    own_picks.start()
    for load in loads:
        load.start()

    barrier = pltpu.get_barrier_semaphore()

    @pl.loop(1, n)
    def _(shift):
        pl.semaphore_signal(
            barrier, inc=1, device_id={"dp": lax.rem(me + shift, n)}, device_id_type=MESH
        )

    own_picks.wait()
    pl.semaphore_wait(barrier, n - 1)

    def pick_copy(target):
        return pltpu.make_async_remote_copy(
            src_ref=all_picks.at[me],
            dst_ref=all_picks.at[me],
            send_sem=pick_send,
            recv_sem=pick_recv.at[my_plane],
            device_id={"dp": target},
            device_id_type=MESH,
        )

    @pl.loop(0, steps)
    def _(step):
        for plane in step_planes(GOING, step):

            @pl.loop(0, PLANE)
            def _(member):
                target = plane * PLANE + member

                @pl.when(target != me)
                def _():
                    pick_copy(target).start()

    matrix = swap_matrix()
    loads[0].wait()
    @pl.loop(0, tok_dev // (2 * SUB))
    def _(block):
        at = pl.multiple_of(block * 2 * SUB, 2 * SUB)
        tiles = to_tiles(matrix, tokens, at)
        for index, tile in enumerate(tiles):
            token_tiles[at + index] = tile

    token_tiles[tok_dev] = jnp.zeros((SUB, LANE), jnp.bfloat16)

    def row_copy(target):
        return pltpu.make_async_remote_copy(
            src_ref=send_buf.at[target],
            dst_ref=recv_buf.at[me],
            send_sem=row_send,
            recv_sem=row_recv.at[my_plane],
            device_id={"dp": target},
            device_id_type=MESH,
        )

    def result_copy(target):
        return pltpu.make_async_remote_copy(
            src_ref=result_buf.at[target],
            dst_ref=return_buf.at[me],
            send_sem=result_send,
            recv_sem=result_recv.at[my_plane],
            device_id={"dp": target},
            device_id_type=MESH,
        )

    own_rows = pltpu.make_async_copy(send_buf.at[me], recv_buf.at[me], local_sem.at[0])
    own_results = pltpu.make_async_copy(result_buf.at[me], return_buf.at[me], local_sem.at[1])

    def send_plane(plane, copy, own):
        @pl.loop(0, PLANE)
        def _(member):
            target = plane * PLANE + member

            @pl.when(target != me)
            def _():
                copy(target).start()

            @pl.when(target == me)
            def _():
                own.start()

    def wait_plane(plane, buffer, semaphores, own):
        @pl.when(plane != my_plane)
        def _():
            part = buffer.at[pl.ds(plane * PLANE, PLANE)]
            pltpu.make_async_copy(part, part, semaphores.at[plane]).wait()

        @pl.when(plane == my_plane)
        def _():
            part = buffer.at[pl.ds(plane * PLANE, PLANE - 1)]
            pltpu.make_async_copy(part, part, semaphores.at[plane]).wait()
            if own is not None:
                own.wait()

    lane = lax.broadcasted_iota(jnp.int32, (PLANE, capacity), 1)
    token_lane = lax.broadcasted_iota(jnp.int32, (PLANE, tok_dev), 1)
    slot_lane = lax.broadcasted_iota(jnp.int32, (PLANE, LANE), 1)

    @pl.loop(0, steps)
    def _(step):
        for plane in step_planes(GOING, step):
            wait_plane(plane, all_picks, pick_recv, None)
            first = pl.multiple_of(plane * PLANE, PLANE)
            picked = all_picks[pl.ds(first, PLANE)].reshape(PLANE, capacity)
            local = picked - me * tok_dev
            mine = (local >= 0) & (local < tok_dev)
            before = jnp.sum((local < 0).astype(jnp.int32), axis=1, keepdims=True)
            place = lane - before
            label = jnp.where(mine, local + 1, 0)
            table = jnp.full((PLANE, LANE), tok_dev, jnp.int32)
            for slot in range(MOST):
                found = jnp.sum(jnp.where(place == slot, label, 0), axis=1, keepdims=True)
                token = jnp.where(found > 0, found - 1, tok_dev)
                table = jnp.where(slot_lane == slot, token, table)
            slots_v[plane] = table
            pltpu.make_async_copy(slots_v.at[plane], slots_s.at[plane], slot_sem).start()
            pltpu.make_async_copy(slots_v.at[plane], slots_s.at[plane], slot_sem).wait()
            for member in range(PLANE):
                for slot in range(MOST):
                    token = jnp.clip(slots_s[plane, member, slot], 0, tok_dev)
                    send_buf[plane * PLANE + member, slot] = token_tiles[token]
            send_plane(plane, row_copy, own_rows)

    loads[1].wait()
    logits = lax.dot_general(
        router[...], tokens[...], (((1,), (1,)), ((), ())), preferred_element_type=jnp.float32
    )
    powers = jnp.exp(logits - jnp.max(logits, axis=0, keepdims=True))
    shares = powers / jnp.sum(powers, axis=0, keepdims=True)
    gates_t[...] = (n * shares).astype(jnp.bfloat16).astype(jnp.float32)

    @pl.loop(0, planes)
    def _(plane):
        gates = gates_t[pl.ds(pl.multiple_of(plane * PLANE, PLANE), PLANE), :]
        table = slots_v[plane]
        for slot in range(MOST):
            at = pl.multiple_of(plane * half + slot * PLANE, PLANE)
            mix_t[pl.ds(at, PLANE), :] = jnp.where(
                token_lane == table[:, slot : slot + 1], gates, 0.0
            )

    mix[...] = mix_t[...].T.astype(jnp.bfloat16)

    for load in loads[2:]:
        load.wait()

    @pl.loop(0, steps)
    def _(step):
        pair = step_planes(COMING, step)
        for plane in pair:
            wait_plane(plane, recv_buf, row_recv, own_rows)
        to_rows(matrix, recv_buf, pair, rows, 0)
        taken = rows[...]
        block = 256
        for at in range(0, gate_w.shape[1], block):
            gate_act = jnp.dot(taken, gate_w[:, at : at + block], preferred_element_type=jnp.float32)
            up_act = jnp.dot(taken, up_w[:, at : at + block], preferred_element_type=jnp.float32)
            hidden[:, at : at + block] = (
                gate_act / (1.0 + jnp.exp(-gate_act)) * up_act
            ).astype(jnp.bfloat16)
        held = hidden[...]
        for at in range(0, width, block):
            result_rows[:, at : at + block] = jnp.dot(
                held, down_w[:, at : at + block], preferred_element_type=jnp.float32
            ).astype(jnp.bfloat16)
        for pack in range(2 * half // (2 * SUB)):
            tiles = to_tiles(matrix, result_rows, pack * 2 * SUB)
            for index, tile in enumerate(tiles):
                row = pack * 2 * SUB + index
                plane = pair[row // half]
                slot, member = divmod(row % half, PLANE)
                result_buf[plane * PLANE + member, slot] = tile
        for plane in pair:
            send_plane(plane, result_copy, own_results)

    @pl.loop(0, steps)
    def _(step):
        for plane in step_planes(COMING, step):
            wait_plane(plane, return_buf, result_recv, own_results)
            to_rows(
                matrix, return_buf, (plane,), return_rows, pl.multiple_of(plane * half, SUB)
            )

    weights = mix[...]
    for at in range(0, width, 256):
        out_ref[:, at : at + 256] = jnp.dot(
            weights, return_rows[:, at : at + 256], preferred_element_type=jnp.float32
        ).astype(jnp.bfloat16)

    def drain(buffer, semaphore):
        part = buffer.at[pl.ds(0, n - 1)]
        pltpu.make_async_copy(part, part, semaphore).wait()

    drain(all_picks, pick_send)
    drain(send_buf, row_send)
    drain(result_buf, result_send)


def layer(n, tokens, router, w_gate, w_up, w_down, picks):
    tok_dev, width = tokens.shape
    hidden_width = w_gate.shape[2]
    capacity = picks.shape[1]
    planes = n // PLANE
    vmem = pl.BlockSpec(memory_space=pltpu.VMEM)
    anywhere = pl.BlockSpec(memory_space=pl.ANY)
    block = (n, MOST, SUB, LANE)
    bf16 = jnp.bfloat16
    group = 2 * PLANE * MOST
    return pl.pallas_call(
        functools.partial(kernel, n),
        out_shape=jax.ShapeDtypeStruct((tok_dev, width), bf16),
        in_specs=[anywhere] * 6,
        out_specs=vmem,
        scratch_shapes=[
            pltpu.VMEM((tok_dev, width), bf16),
            pltpu.VMEM(router.shape[::-1], bf16),
            pltpu.VMEM((width, hidden_width), bf16),
            pltpu.VMEM((width, hidden_width), bf16),
            pltpu.VMEM((hidden_width, width), bf16),
            pltpu.VMEM((tok_dev + 1, SUB, LANE), bf16),
            pltpu.VMEM((n, tok_dev), jnp.float32),
            pltpu.VMEM((n, 1, capacity), jnp.int32),
            pltpu.VMEM((planes, PLANE, LANE), jnp.int32),
            pltpu.SMEM((planes, PLANE, LANE), jnp.int32),
            pltpu.VMEM((n * MOST, tok_dev), jnp.float32),
            pltpu.VMEM((tok_dev, n * MOST), bf16),
            pltpu.VMEM(block, bf16),
            pltpu.VMEM(block, bf16),
            pltpu.VMEM((group, width), bf16),
            pltpu.VMEM((group, hidden_width), bf16),
            pltpu.VMEM((group, width), bf16),
            pltpu.VMEM(block, bf16),
            pltpu.VMEM(block, bf16),
            pltpu.VMEM((n * MOST, width), bf16),
            pltpu.SemaphoreType.DMA((5,)),
            pltpu.SemaphoreType.DMA,
            pltpu.SemaphoreType.DMA((3,)),
            pltpu.SemaphoreType.DMA,
            pltpu.SemaphoreType.DMA((planes,)),
            pltpu.SemaphoreType.DMA,
            pltpu.SemaphoreType.DMA((planes,)),
            pltpu.SemaphoreType.DMA,
            pltpu.SemaphoreType.DMA((planes,)),
        ],
        compiler_params=pltpu.CompilerParams(
            collective_id=0, has_side_effects=True, vmem_limit_bytes=32 * 2**20
        ),
    )(
        *[
            pltpu.with_memory_space_constraint(operand, pltpu.HBM)
            for operand in (tokens, router.T, w_gate, w_up, w_down, picks)
        ]
    )


def solution(mesh):
    n = mesh.shape["dp"]
    return jax.shard_map(
        functools.partial(layer, n),
        mesh=mesh,
        in_specs=(
            P(("rep", "dp"), None),
            P("rep", None),
            P("dp", None, None),
            P("dp", None, None),
            P("dp", None, None),
            P(("rep", "dp"), None),
        ),
        out_specs=P(("rep", "dp"), None),
        check_vma=False,
    )
```

```python
import functools

import jax
import jax.numpy as jnp
from jax import lax
from jax.experimental import pallas as pl
from jax.experimental.pallas import tpu as pltpu
from jax.sharding import PartitionSpec as P

MOST = 6
PLANE = 8
SUB, LANE = 16, 128
MESH = pl.DeviceIdType.MESH
GOING = ((1, 7), (2, 6), (3, 5), (4, 0))
COMING = ((1, 7), (2, 6), (3, 5), (4, 0))


def swap_matrix():
    row = lax.broadcasted_iota(jnp.int32, (SUB * SUB, SUB * SUB), 0)
    col = lax.broadcasted_iota(jnp.int32, (SUB * SUB, SUB * SUB), 1)
    swapped = (col % SUB) * SUB + col // SUB
    return (row == swapped).astype(jnp.float32).astype(jnp.bfloat16)


def swap(matrix, stacked):
    return jnp.dot(matrix, stacked, preferred_element_type=jnp.float32).astype(jnp.bfloat16)


def plane_tiles(buffer, plane, part):
    tiles = [
        buffer[plane * PLANE + member, 2 * part + half]
        for half in range(2)
        for member in range(PLANE)
    ]
    return jnp.concatenate(tiles, axis=0)


def to_rows(matrix, buffer, planes, target, target_row):
    jobs = [(plane, part) for plane in planes for part in range(MOST // 2)]
    for first in range(0, len(jobs), 2):
        pair = jobs[first : first + 2]
        stacked = jnp.concatenate([plane_tiles(buffer, *job) for job in pair], axis=1)
        moved = swap(matrix, stacked)
        for which in range(len(pair)):
            at = target_row + (first + which) * SUB
            for chunk in range(SUB):
                target[pl.ds(at, SUB), chunk * LANE : (chunk + 1) * LANE] = moved[
                    chunk * SUB : (chunk + 1) * SUB, which * LANE : (which + 1) * LANE
                ]


def to_tiles(matrix, rows, first_row):
    def stack(at):
        return jnp.concatenate(
            [rows[pl.ds(at, SUB), chunk * LANE : (chunk + 1) * LANE] for chunk in range(SUB)],
            axis=0,
        )

    stacked = jnp.concatenate([stack(first_row), stack(first_row + SUB)], axis=1)
    moved = swap(matrix, stacked)
    return [
        moved[row * SUB : (row + 1) * SUB, half * LANE : (half + 1) * LANE]
        for half in range(2)
        for row in range(SUB)
    ]


def kernel(
    n,
    tokens_hbm,
    router_hbm,
    gate_hbm,
    up_hbm,
    down_hbm,
    picks_hbm,
    out_ref,
    tokens,
    router,
    gate_w,
    up_w,
    down_w,
    token_tiles,
    gates_t,
    picks,
    chosen,
    slots_v,
    slots_s,
    mix_t,
    mix,
    send_buf,
    recv_buf,
    rows,
    hidden,
    result_rows,
    result_buf,
    return_buf,
    return_rows,
    load_sem,
    slot_sem,
    local_sem,
    pick_send,
    pick_recv,
    row_send,
    row_recv,
    result_send,
    result_recv,
):
    me = lax.axis_index("dp")
    planes = n // PLANE
    my_plane = me // PLANE
    tok_dev, width = tokens.shape
    capacity = picks.shape[1]
    steps = planes // 2
    my_member = lax.rem(me, PLANE)
    half = PLANE * MOST

    def peer(plane, turn):
        column = lax.rem(my_member // 2 + turn // 2, PLANE // 2)
        core = lax.rem(my_member + turn, 2)
        return plane * PLANE + column * 2 + core

    def step_planes(order, step):
        pair = order[-1]
        for index in range(steps - 1):
            pair = [jnp.where(step == index, *both) for both in zip(order[index], pair)]
        return [lax.rem(my_plane + distance, planes) for distance in pair]

    loads = [
        pltpu.make_async_copy(tokens_hbm, tokens, load_sem.at[0]),
        pltpu.make_async_copy(router_hbm, router, load_sem.at[1]),
        pltpu.make_async_copy(gate_hbm.at[0], gate_w, load_sem.at[2]),
        pltpu.make_async_copy(up_hbm.at[0], up_w, load_sem.at[3]),
        pltpu.make_async_copy(down_hbm.at[0], down_w, load_sem.at[4]),
    ]
    own_picks = pltpu.make_async_copy(picks_hbm, picks, local_sem.at[2])
    own_picks.start()
    for load in loads[:2]:
        load.start()

    barrier = pltpu.get_barrier_semaphore()

    @pl.loop(1, n)
    def _(shift):
        pl.semaphore_signal(
            barrier, inc=1, device_id={"dp": lax.rem(me + shift, n)}, device_id_type=MESH
        )

    def send_picks(distance):
        plane = lax.rem(my_plane + distance, planes)

        @pl.loop(0, PLANE)
        def _(turn):
            target = peer(plane, turn)

            @pl.when(target != me)
            def _():
                pltpu.make_async_remote_copy(
                    src_ref=chosen.at[target],
                    dst_ref=slots_s.at[me],
                    send_sem=pick_send,
                    recv_sem=pick_recv.at[my_plane],
                    device_id={"dp": target},
                    device_id_type=MESH,
                ).start()

    own_picks.wait()
    owner = lax.broadcasted_iota(jnp.int32, (n, capacity), 0)
    lane = lax.broadcasted_iota(jnp.int32, (n, capacity), 1)
    slot_lane = lax.broadcasted_iota(jnp.int32, (n, LANE), 1)
    local = picks[...] - owner * tok_dev
    before = jnp.sum((local < 0).astype(jnp.int32), axis=1, keepdims=True)
    place = lane - before
    label = jnp.where((local >= 0) & (local < tok_dev), local + 1, 0)
    table = jnp.full((n, LANE), tok_dev, jnp.int32)
    for slot in range(MOST):
        found = jnp.sum(jnp.where(place == slot, label, 0), axis=1, keepdims=True)
        table = jnp.where(slot_lane == slot, jnp.where(found > 0, found - 1, tok_dev), table)
    chosen[...] = table.reshape(n, 1, LANE)

    pl.semaphore_wait(barrier, n - 1)
    own_slots = pltpu.make_async_copy(chosen.at[me], slots_s.at[me], local_sem.at[2])
    own_slots.start()

    @pl.loop(0, planes)
    def _(turn):
        up, down = step_planes(GOING, turn // 2)
        send_picks(jnp.where(turn % 2 == 0, up, down) - my_plane + planes)


    matrix = swap_matrix()
    loads[0].wait()
    @pl.loop(0, tok_dev // (2 * SUB))
    def _(block):
        at = pl.multiple_of(block * 2 * SUB, 2 * SUB)
        tiles = to_tiles(matrix, tokens, at)
        for index, tile in enumerate(tiles):
            token_tiles[at + index] = tile

    token_tiles[tok_dev] = jnp.zeros((SUB, LANE), jnp.bfloat16)
    for load in loads[2:]:
        load.start()

    def row_copy(target):
        return pltpu.make_async_remote_copy(
            src_ref=send_buf.at[target],
            dst_ref=recv_buf.at[me],
            send_sem=row_send,
            recv_sem=row_recv.at[my_plane],
            device_id={"dp": target},
            device_id_type=MESH,
        )

    def result_copy(target):
        return pltpu.make_async_remote_copy(
            src_ref=result_buf.at[target],
            dst_ref=return_buf.at[me],
            send_sem=result_send,
            recv_sem=result_recv.at[my_plane],
            device_id={"dp": target},
            device_id_type=MESH,
        )

    own_rows = pltpu.make_async_copy(send_buf.at[me], recv_buf.at[me], local_sem.at[0])
    own_results = pltpu.make_async_copy(result_buf.at[me], return_buf.at[me], local_sem.at[1])

    def send_plane(plane, copy, own, turned):
        @pl.loop(0, PLANE)
        def _(turn):
            target = peer(plane, turn) if turned else plane * PLANE + turn

            @pl.when(target != me)
            def _():
                copy(target).start()

            @pl.when(target == me)
            def _():
                own.start()

    def wait_plane(plane, buffer, semaphores, own):
        @pl.when(plane != my_plane)
        def _():
            part = buffer.at[pl.ds(plane * PLANE, PLANE)]
            pltpu.make_async_copy(part, part, semaphores.at[plane]).wait()

        @pl.when(plane == my_plane)
        def _():
            part = buffer.at[pl.ds(plane * PLANE, PLANE - 1)]
            pltpu.make_async_copy(part, part, semaphores.at[plane]).wait()
            if own is not None:
                own.wait()

    token_lane = lax.broadcasted_iota(jnp.int32, (PLANE, tok_dev), 1)

    def serve(plane):
        wait_plane(plane, slots_s, pick_recv, own_slots)

        @pl.loop(0, PLANE)
        def _(member):
            for slot in range(MOST):
                token = jnp.clip(slots_s[plane * PLANE + member, 0, slot], 0, tok_dev)
                send_buf[plane * PLANE + member, slot] = token_tiles[token]

        send_plane(plane, row_copy, own_rows, True)

    @pl.loop(0, 2 * steps)
    def _(turn):
        step = turn // 2

        up, down = step_planes(GOING, step)
        serve(jnp.where(turn % 2 == 0, up, down))

    slots_copy = pltpu.make_async_copy(slots_s, slots_v, slot_sem)
    slots_copy.start()
    loads[1].wait()
    logits = lax.dot_general(
        router[...], tokens[...], (((1,), (1,)), ((), ())), preferred_element_type=jnp.float32
    )
    powers = jnp.exp(logits - jnp.max(logits, axis=0, keepdims=True))
    shares = powers / jnp.sum(powers, axis=0, keepdims=True)
    gates_t[...] = (n * shares).astype(jnp.bfloat16).astype(jnp.float32)

    slots_copy.wait()

    @pl.loop(0, planes)
    def _(plane):
        gates = gates_t[pl.ds(pl.multiple_of(plane * PLANE, PLANE), PLANE), :]
        table = slots_v[pl.ds(plane * PLANE, PLANE)].reshape(PLANE, LANE)
        for slot in range(MOST):
            at = pl.multiple_of(plane * half + slot * PLANE, PLANE)
            mix_t[pl.ds(at, PLANE), :] = jnp.where(
                token_lane == table[:, slot : slot + 1], gates, 0.0
            )

    mix[...] = mix_t[...].T.astype(jnp.bfloat16)

    for load in loads[2:]:
        load.wait()

    @pl.loop(0, steps)
    def _(step):
        pair = step_planes(COMING, step)
        for plane in pair:
            wait_plane(plane, recv_buf, row_recv, own_rows)
        to_rows(matrix, recv_buf, pair, rows, 0)
        taken = rows[...]
        block = 256
        for at in range(0, gate_w.shape[1], block):
            gate_act = jnp.dot(taken, gate_w[:, at : at + block], preferred_element_type=jnp.float32)
            up_act = jnp.dot(taken, up_w[:, at : at + block], preferred_element_type=jnp.float32)
            hidden[:, at : at + block] = (
                gate_act / (1.0 + jnp.exp(-gate_act)) * up_act
            ).astype(jnp.bfloat16)
        held = hidden[...]
        for at in range(0, width, block):
            result_rows[:, at : at + block] = jnp.dot(
                held, down_w[:, at : at + block], preferred_element_type=jnp.float32
            ).astype(jnp.bfloat16)
        for pack in range(2 * half // (2 * SUB)):
            tiles = to_tiles(matrix, result_rows, pack * 2 * SUB)
            for index, tile in enumerate(tiles):
                row = pack * 2 * SUB + index
                plane = pair[row // half]
                slot, member = divmod(row % half, PLANE)
                result_buf[plane * PLANE + member, slot] = tile
        for plane in pair:
            send_plane(plane, result_copy, own_results, False)

    @pl.loop(0, steps)
    def _(step):
        for plane in step_planes(COMING, step):
            wait_plane(plane, return_buf, result_recv, own_results)
            to_rows(
                matrix, return_buf, (plane,), return_rows, pl.multiple_of(plane * half, SUB)
            )

    weights = mix[...]
    for at in range(0, width, 256):
        out_ref[:, at : at + 256] = jnp.dot(
            weights, return_rows[:, at : at + 256], preferred_element_type=jnp.float32
        ).astype(jnp.bfloat16)

    def drain(buffer, semaphore):
        part = buffer.at[pl.ds(0, n - 1)]
        pltpu.make_async_copy(part, part, semaphore).wait()

    drain(chosen, pick_send)
    drain(send_buf, row_send)
    drain(result_buf, result_send)


def layer(n, tokens, router, w_gate, w_up, w_down, picks):
    tok_dev, width = tokens.shape
    hidden_width = w_gate.shape[2]
    capacity = picks.shape[1]
    planes = n // PLANE
    vmem = pl.BlockSpec(memory_space=pltpu.VMEM)
    anywhere = pl.BlockSpec(memory_space=pl.ANY)
    block = (n, MOST, SUB, LANE)
    bf16 = jnp.bfloat16
    group = 2 * PLANE * MOST
    return pl.pallas_call(
        functools.partial(kernel, n),
        out_shape=jax.ShapeDtypeStruct((tok_dev, width), bf16),
        in_specs=[anywhere] * 6,
        out_specs=vmem,
        scratch_shapes=[
            pltpu.VMEM((tok_dev, width), bf16),
            pltpu.VMEM(router.shape[::-1], bf16),
            pltpu.VMEM((width, hidden_width), bf16),
            pltpu.VMEM((width, hidden_width), bf16),
            pltpu.VMEM((hidden_width, width), bf16),
            pltpu.VMEM((tok_dev + 1, SUB, LANE), bf16),
            pltpu.VMEM((n, tok_dev), jnp.float32),
            pltpu.VMEM((1, capacity), jnp.int32),
            pltpu.VMEM((n, 1, LANE), jnp.int32),
            pltpu.VMEM((n, 1, LANE), jnp.int32),
            pltpu.SMEM((n, 1, LANE), jnp.int32),
            pltpu.VMEM((n * MOST, tok_dev), jnp.float32),
            pltpu.VMEM((tok_dev, n * MOST), bf16),
            pltpu.VMEM(block, bf16),
            pltpu.VMEM(block, bf16),
            pltpu.VMEM((group, width), bf16),
            pltpu.VMEM((group, hidden_width), bf16),
            pltpu.VMEM((group, width), bf16),
            pltpu.VMEM(block, bf16),
            pltpu.VMEM(block, bf16),
            pltpu.VMEM((n * MOST, width), bf16),
            pltpu.SemaphoreType.DMA((5,)),
            pltpu.SemaphoreType.DMA,
            pltpu.SemaphoreType.DMA((3,)),
            pltpu.SemaphoreType.DMA,
            pltpu.SemaphoreType.DMA((planes,)),
            pltpu.SemaphoreType.DMA,
            pltpu.SemaphoreType.DMA((planes,)),
            pltpu.SemaphoreType.DMA,
            pltpu.SemaphoreType.DMA((planes,)),
        ],
        compiler_params=pltpu.CompilerParams(
            collective_id=0, has_side_effects=True, vmem_limit_bytes=32 * 2**20
        ),
    )(
        *[
            pltpu.with_memory_space_constraint(operand, pltpu.HBM)
            for operand in (tokens, router.T, w_gate, w_up, w_down, picks)
        ]
    )


def solution(mesh):
    n = mesh.shape["dp"]
    return jax.shard_map(
        functools.partial(layer, n),
        mesh=mesh,
        in_specs=(
            P(("rep", "dp"), None),
            P("rep", None),
            P("dp", None, None),
            P("dp", None, None),
            P("dp", None, None),
            P(("rep", "dp"), None),
        ),
        out_specs=P(("rep", "dp"), None),
        check_vma=False,
    )
```

```python
import functools

import jax
import jax.numpy as jnp
from jax import lax
from jax.experimental import pallas as pl
from jax.experimental.pallas import tpu as pltpu
from jax.sharding import PartitionSpec as P

MOST = 6
PLANE = 8
SUB, LANE = 16, 128
MESH = pl.DeviceIdType.MESH
GOING = ((1, 7), (4, 0), (3, 5), (2, 6))
COMING = ((1, 7), (4, 0), (3, 5), (2, 6))


def swap_matrix():
    row = lax.broadcasted_iota(jnp.int32, (SUB * SUB, SUB * SUB), 0)
    col = lax.broadcasted_iota(jnp.int32, (SUB * SUB, SUB * SUB), 1)
    swapped = (col % SUB) * SUB + col // SUB
    return (row == swapped).astype(jnp.float32).astype(jnp.bfloat16)


def swap(matrix, stacked):
    return jnp.dot(matrix, stacked, preferred_element_type=jnp.float32).astype(jnp.bfloat16)


def plane_tiles(buffer, plane, part):
    tiles = [
        buffer[plane * PLANE + member, 2 * part + half]
        for half in range(2)
        for member in range(PLANE)
    ]
    return jnp.concatenate(tiles, axis=0)


def to_rows(matrix, buffer, planes, target, target_row):
    jobs = [(plane, part) for plane in planes for part in range(MOST // 2)]
    for first in range(0, len(jobs), 2):
        pair = jobs[first : first + 2]
        stacked = jnp.concatenate([plane_tiles(buffer, *job) for job in pair], axis=1)
        moved = swap(matrix, stacked)
        for which in range(len(pair)):
            at = target_row + (first + which) * SUB
            for chunk in range(SUB):
                target[pl.ds(at, SUB), chunk * LANE : (chunk + 1) * LANE] = moved[
                    chunk * SUB : (chunk + 1) * SUB, which * LANE : (which + 1) * LANE
                ]


def to_tiles(matrix, rows, first_row):
    def stack(at):
        return jnp.concatenate(
            [rows[pl.ds(at, SUB), chunk * LANE : (chunk + 1) * LANE] for chunk in range(SUB)],
            axis=0,
        )

    stacked = jnp.concatenate([stack(first_row), stack(first_row + SUB)], axis=1)
    moved = swap(matrix, stacked)
    return [
        moved[row * SUB : (row + 1) * SUB, half * LANE : (half + 1) * LANE]
        for half in range(2)
        for row in range(SUB)
    ]


def kernel(
    n,
    tokens_hbm,
    router_hbm,
    gate_hbm,
    up_hbm,
    down_hbm,
    picks_hbm,
    out_ref,
    tokens,
    router,
    gate_w,
    up_w,
    down_w,
    token_tiles,
    gates_t,
    picks,
    chosen,
    slots_v,
    slots_s,
    mix_t,
    mix,
    send_buf,
    recv_buf,
    rows,
    hidden,
    result_rows,
    result_buf,
    return_buf,
    return_rows,
    load_sem,
    slot_sem,
    local_sem,
    pick_send,
    pick_recv,
    row_send,
    row_recv,
    result_send,
    result_recv,
):
    me = lax.axis_index("dp")
    planes = n // PLANE
    my_plane = me // PLANE
    tok_dev, width = tokens.shape
    capacity = picks.shape[1]
    steps = planes // 2
    my_member = lax.rem(me, PLANE)
    half = PLANE * MOST

    def peer(plane, turn):
        column = lax.rem(my_member // 2 + turn // 2, PLANE // 2)
        core = lax.rem(my_member + turn, 2)
        return plane * PLANE + column * 2 + core

    def step_planes(order, step):
        pair = order[-1]
        for index in range(steps - 1):
            pair = [jnp.where(step == index, *both) for both in zip(order[index], pair)]
        return [lax.rem(my_plane + distance, planes) for distance in pair]

    loads = [
        pltpu.make_async_copy(tokens_hbm, tokens, load_sem.at[0]),
        pltpu.make_async_copy(router_hbm, router, load_sem.at[1]),
        pltpu.make_async_copy(gate_hbm.at[0], gate_w, load_sem.at[2]),
        pltpu.make_async_copy(up_hbm.at[0], up_w, load_sem.at[3]),
        pltpu.make_async_copy(down_hbm.at[0], down_w, load_sem.at[4]),
    ]
    own_picks = pltpu.make_async_copy(picks_hbm, picks, local_sem.at[2])
    own_picks.start()
    for load in loads[:2]:
        load.start()

    barrier = pltpu.get_barrier_semaphore()

    @pl.loop(1, n)
    def _(shift):
        pl.semaphore_signal(
            barrier, inc=1, device_id={"dp": lax.rem(me + shift, n)}, device_id_type=MESH
        )

    def send_picks(distance):
        plane = lax.rem(my_plane + distance, planes)

        @pl.loop(0, PLANE)
        def _(turn):
            target = peer(plane, turn)

            @pl.when(target != me)
            def _():
                pltpu.make_async_remote_copy(
                    src_ref=chosen.at[target],
                    dst_ref=slots_s.at[me],
                    send_sem=pick_send,
                    recv_sem=pick_recv.at[my_plane],
                    device_id={"dp": target},
                    device_id_type=MESH,
                ).start()

    own_picks.wait()
    owner = lax.broadcasted_iota(jnp.int32, (n, capacity), 0)
    lane = lax.broadcasted_iota(jnp.int32, (n, capacity), 1)
    slot_lane = lax.broadcasted_iota(jnp.int32, (n, LANE), 1)
    local = picks[...] - owner * tok_dev
    before = jnp.sum((local < 0).astype(jnp.int32), axis=1, keepdims=True)
    place = lane - before
    label = jnp.where((local >= 0) & (local < tok_dev), local + 1, 0)
    table = jnp.full((n, LANE), tok_dev, jnp.int32)
    for slot in range(MOST):
        found = jnp.sum(jnp.where(place == slot, label, 0), axis=1, keepdims=True)
        table = jnp.where(slot_lane == slot, jnp.where(found > 0, found - 1, tok_dev), table)
    chosen[...] = table.reshape(n, 1, LANE)

    pl.semaphore_wait(barrier, n - 1)
    own_slots = pltpu.make_async_copy(chosen.at[me], slots_s.at[me], local_sem.at[2])
    own_slots.start()

    @pl.loop(0, planes)
    def _(turn):
        up, down = step_planes(GOING, turn // 2)
        send_picks(jnp.where(turn % 2 == 0, up, down) - my_plane + planes)


    matrix = swap_matrix()
    loads[0].wait()
    @pl.loop(0, tok_dev // (2 * SUB))
    def _(block):
        at = pl.multiple_of(block * 2 * SUB, 2 * SUB)
        tiles = to_tiles(matrix, tokens, at)
        for index, tile in enumerate(tiles):
            token_tiles[at + index] = tile

    token_tiles[tok_dev] = jnp.zeros((SUB, LANE), jnp.bfloat16)
    for load in loads[2:]:
        load.start()

    def row_copy(target):
        return pltpu.make_async_remote_copy(
            src_ref=send_buf.at[target],
            dst_ref=recv_buf.at[me],
            send_sem=row_send,
            recv_sem=row_recv.at[my_plane],
            device_id={"dp": target},
            device_id_type=MESH,
        )

    def result_copy(target):
        return pltpu.make_async_remote_copy(
            src_ref=result_buf.at[target],
            dst_ref=return_buf.at[me],
            send_sem=result_send,
            recv_sem=result_recv.at[my_plane],
            device_id={"dp": target},
            device_id_type=MESH,
        )

    own_rows = pltpu.make_async_copy(send_buf.at[me], recv_buf.at[me], local_sem.at[0])
    own_results = pltpu.make_async_copy(result_buf.at[me], return_buf.at[me], local_sem.at[1])

    def send_plane(plane, copy, own, turned):
        @pl.loop(0, PLANE)
        def _(turn):
            target = peer(plane, turn) if turned else plane * PLANE + (turn // 2 + jnp.where(turn >= 6, -1, jnp.where(turn >= 4, 1, 0))) * 2 + turn % 2

            @pl.when(target != me)
            def _():
                copy(target).start()

            @pl.when(target == me)
            def _():
                own.start()

    def wait_plane(plane, buffer, semaphores, own):
        @pl.when(plane != my_plane)
        def _():
            part = buffer.at[pl.ds(plane * PLANE, PLANE)]
            pltpu.make_async_copy(part, part, semaphores.at[plane]).wait()

        @pl.when(plane == my_plane)
        def _():
            part = buffer.at[pl.ds(plane * PLANE, PLANE - 1)]
            pltpu.make_async_copy(part, part, semaphores.at[plane]).wait()
            if own is not None:
                own.wait()

    token_lane = lax.broadcasted_iota(jnp.int32, (PLANE, tok_dev), 1)

    def serve(plane):
        wait_plane(plane, slots_s, pick_recv, own_slots)

        @pl.loop(0, PLANE)
        def _(member):
            for slot in range(MOST):
                token = jnp.clip(slots_s[plane * PLANE + member, 0, slot], 0, tok_dev)
                send_buf[plane * PLANE + member, slot] = token_tiles[token]

        send_plane(plane, row_copy, own_rows, True)

    @pl.loop(0, 2 * steps)
    def _(turn):
        step = turn // 2

        up, down = step_planes(GOING, step)
        serve(jnp.where(turn % 2 == 0, up, down))

    slots_copy = pltpu.make_async_copy(slots_s, slots_v, slot_sem)
    slots_copy.start()
    loads[1].wait()
    logits = lax.dot_general(
        router[...], tokens[...], (((1,), (1,)), ((), ())), preferred_element_type=jnp.float32
    )
    powers = jnp.exp(logits - jnp.max(logits, axis=0, keepdims=True))
    shares = powers / jnp.sum(powers, axis=0, keepdims=True)
    gates_t[...] = (n * shares).astype(jnp.bfloat16).astype(jnp.float32)

    slots_copy.wait()

    @pl.loop(0, planes)
    def _(plane):
        gates = gates_t[pl.ds(pl.multiple_of(plane * PLANE, PLANE), PLANE), :]
        table = slots_v[pl.ds(plane * PLANE, PLANE)].reshape(PLANE, LANE)
        for slot in range(MOST):
            at = pl.multiple_of(plane * half + slot * PLANE, PLANE)
            mix_t[pl.ds(at, PLANE), :] = jnp.where(
                token_lane == table[:, slot : slot + 1], gates, 0.0
            )

    mix[...] = mix_t[...].T.astype(jnp.bfloat16)

    for load in loads[2:]:
        load.wait()

    @pl.loop(0, steps)
    def _(step):
        pair = step_planes(COMING, step)
        for plane in pair:
            wait_plane(plane, recv_buf, row_recv, own_rows)
        to_rows(matrix, recv_buf, pair, rows, 0)
        taken = rows[...]
        block = 256
        for at in range(0, gate_w.shape[1], block):
            gate_act = jnp.dot(taken, gate_w[:, at : at + block], preferred_element_type=jnp.float32)
            up_act = jnp.dot(taken, up_w[:, at : at + block], preferred_element_type=jnp.float32)
            hidden[:, at : at + block] = (
                gate_act / (1.0 + jnp.exp(-gate_act)) * up_act
            ).astype(jnp.bfloat16)
        held = hidden[...]
        for at in range(0, width, block):
            result_rows[:, at : at + block] = jnp.dot(
                held, down_w[:, at : at + block], preferred_element_type=jnp.float32
            ).astype(jnp.bfloat16)
        for pack in range(2 * half // (2 * SUB)):
            tiles = to_tiles(matrix, result_rows, pack * 2 * SUB)
            for index, tile in enumerate(tiles):
                row = pack * 2 * SUB + index
                plane = pair[row // half]
                slot, member = divmod(row % half, PLANE)
                result_buf[plane * PLANE + member, slot] = tile
        for plane in pair:
            send_plane(plane, result_copy, own_results, False)

    @pl.loop(0, steps)
    def _(step):
        for plane in step_planes(COMING, step):
            wait_plane(plane, return_buf, result_recv, own_results)
            to_rows(
                matrix, return_buf, (plane,), return_rows, pl.multiple_of(plane * half, SUB)
            )

    weights = mix[...]
    for at in range(0, width, 256):
        out_ref[:, at : at + 256] = jnp.dot(
            weights, return_rows[:, at : at + 256], preferred_element_type=jnp.float32
        ).astype(jnp.bfloat16)

    def drain(buffer, semaphore):
        part = buffer.at[pl.ds(0, n - 1)]
        pltpu.make_async_copy(part, part, semaphore).wait()

    drain(chosen, pick_send)
    drain(send_buf, row_send)
    drain(result_buf, result_send)


def layer(n, tokens, router, w_gate, w_up, w_down, picks):
    tok_dev, width = tokens.shape
    hidden_width = w_gate.shape[2]
    capacity = picks.shape[1]
    planes = n // PLANE
    vmem = pl.BlockSpec(memory_space=pltpu.VMEM)
    anywhere = pl.BlockSpec(memory_space=pl.ANY)
    block = (n, MOST, SUB, LANE)
    bf16 = jnp.bfloat16
    group = 2 * PLANE * MOST
    return pl.pallas_call(
        functools.partial(kernel, n),
        out_shape=jax.ShapeDtypeStruct((tok_dev, width), bf16),
        in_specs=[anywhere] * 6,
        out_specs=vmem,
        scratch_shapes=[
            pltpu.VMEM((tok_dev, width), bf16),
            pltpu.VMEM(router.shape[::-1], bf16),
            pltpu.VMEM((width, hidden_width), bf16),
            pltpu.VMEM((width, hidden_width), bf16),
            pltpu.VMEM((hidden_width, width), bf16),
            pltpu.VMEM((tok_dev + 1, SUB, LANE), bf16),
            pltpu.VMEM((n, tok_dev), jnp.float32),
            pltpu.VMEM((1, capacity), jnp.int32),
            pltpu.VMEM((n, 1, LANE), jnp.int32),
            pltpu.VMEM((n, 1, LANE), jnp.int32),
            pltpu.SMEM((n, 1, LANE), jnp.int32),
            pltpu.VMEM((n * MOST, tok_dev), jnp.float32),
            pltpu.VMEM((tok_dev, n * MOST), bf16),
            pltpu.VMEM(block, bf16),
            pltpu.VMEM(block, bf16),
            pltpu.VMEM((group, width), bf16),
            pltpu.VMEM((group, hidden_width), bf16),
            pltpu.VMEM((group, width), bf16),
            pltpu.VMEM(block, bf16),
            pltpu.VMEM(block, bf16),
            pltpu.VMEM((n * MOST, width), bf16),
            pltpu.SemaphoreType.DMA((5,)),
            pltpu.SemaphoreType.DMA,
            pltpu.SemaphoreType.DMA((3,)),
            pltpu.SemaphoreType.DMA,
            pltpu.SemaphoreType.DMA((planes,)),
            pltpu.SemaphoreType.DMA,
            pltpu.SemaphoreType.DMA((planes,)),
            pltpu.SemaphoreType.DMA,
            pltpu.SemaphoreType.DMA((planes,)),
        ],
        compiler_params=pltpu.CompilerParams(
            collective_id=0, has_side_effects=True, vmem_limit_bytes=32 * 2**20
        ),
    )(
        *[
            pltpu.with_memory_space_constraint(operand, pltpu.HBM)
            for operand in (tokens, router.T, w_gate, w_up, w_down, picks)
        ]
    )


def solution(mesh):
    n = mesh.shape["dp"]
    return jax.shard_map(
        functools.partial(layer, n),
        mesh=mesh,
        in_specs=(
            P(("rep", "dp"), None),
            P("rep", None),
            P("dp", None, None),
            P("dp", None, None),
            P("dp", None, None),
            P(("rep", "dp"), None),
        ),
        out_specs=P(("rep", "dp"), None),
        check_vma=False,
    )
```

```python
import functools

import jax
import jax.numpy as jnp
from jax import lax
from jax.experimental import pallas as pl
from jax.experimental.pallas import tpu as pltpu
from jax.sharding import PartitionSpec as P

BLOCK = 512
MOST = 6
PLANE = 8
SUB, LANE = 16, 128
MESH = pl.DeviceIdType.MESH
GOING = ((1, 7), (4, 0), (3, 5), (2, 6))
COMING = ((1, 7), (4, 0), (3, 5), (2, 6))


def swap_matrix():
    row = lax.broadcasted_iota(jnp.int32, (SUB * SUB, SUB * SUB), 0)
    col = lax.broadcasted_iota(jnp.int32, (SUB * SUB, SUB * SUB), 1)
    swapped = (col % SUB) * SUB + col // SUB
    return (row == swapped).astype(jnp.float32).astype(jnp.bfloat16)


def swap(matrix, stacked):
    return jnp.dot(matrix, stacked, preferred_element_type=jnp.float32).astype(jnp.bfloat16)


def plane_tiles(buffer, plane, part):
    tiles = [
        buffer[plane * PLANE + member, 2 * part + half]
        for half in range(2)
        for member in range(PLANE)
    ]
    return jnp.concatenate(tiles, axis=0)


def to_rows(matrix, buffer, planes, target, target_row):
    jobs = [(plane, part) for plane in planes for part in range(MOST // 2)]
    for first in range(0, len(jobs), 2):
        pair = jobs[first : first + 2]
        stacked = jnp.concatenate([plane_tiles(buffer, *job) for job in pair], axis=1)
        moved = swap(matrix, stacked)
        for which in range(len(pair)):
            at = target_row + (first + which) * SUB
            for chunk in range(SUB):
                target[pl.ds(at, SUB), chunk * LANE : (chunk + 1) * LANE] = moved[
                    chunk * SUB : (chunk + 1) * SUB, which * LANE : (which + 1) * LANE
                ]


def to_tiles(matrix, rows, first_row):
    def stack(at):
        return jnp.concatenate(
            [rows[pl.ds(at, SUB), chunk * LANE : (chunk + 1) * LANE] for chunk in range(SUB)],
            axis=0,
        )

    stacked = jnp.concatenate([stack(first_row), stack(first_row + SUB)], axis=1)
    moved = swap(matrix, stacked)
    return [
        moved[row * SUB : (row + 1) * SUB, half * LANE : (half + 1) * LANE]
        for half in range(2)
        for row in range(SUB)
    ]


def kernel(
    n,
    tokens_hbm,
    router_hbm,
    gate_hbm,
    up_hbm,
    down_hbm,
    picks_hbm,
    return_rows,
    mix,
    tokens,
    router,
    gate_w,
    up_w,
    down_w,
    token_tiles,
    gates_t,
    picks,
    chosen,
    slots_v,
    slots_s,
    mix_t,
    send_buf,
    recv_buf,
    rows,
    hidden,
    result_rows,
    result_buf,
    return_buf,
    load_sem,
    slot_sem,
    local_sem,
    pick_send,
    pick_recv,
    row_send,
    row_recv,
    result_send,
    result_recv,
):
    me = lax.axis_index("dp")
    planes = n // PLANE
    my_plane = me // PLANE
    tok_dev, width = tokens.shape
    capacity = picks.shape[1]
    steps = planes // 2
    my_member = lax.rem(me, PLANE)
    half = PLANE * MOST

    def peer(plane, turn):
        column = lax.rem(my_member // 2 + turn // 2, PLANE // 2)
        core = lax.rem(my_member + turn, 2)
        return plane * PLANE + column * 2 + core

    def step_planes(order, step):
        pair = order[-1]
        for index in range(steps - 1):
            pair = [jnp.where(step == index, *both) for both in zip(order[index], pair)]
        return [lax.rem(my_plane + distance, planes) for distance in pair]

    loads = [
        pltpu.make_async_copy(tokens_hbm, tokens, load_sem.at[0]),
        pltpu.make_async_copy(router_hbm, router, load_sem.at[1]),
        pltpu.make_async_copy(gate_hbm.at[0], gate_w, load_sem.at[2]),
        pltpu.make_async_copy(up_hbm.at[0], up_w, load_sem.at[3]),
        pltpu.make_async_copy(down_hbm.at[0], down_w, load_sem.at[4]),
    ]
    own_picks = pltpu.make_async_copy(picks_hbm, picks, local_sem.at[2])
    own_picks.start()
    for load in loads[:2]:
        load.start()

    barrier = pltpu.get_barrier_semaphore()

    @pl.loop(1, n)
    def _(shift):
        pl.semaphore_signal(
            barrier, inc=1, device_id={"dp": lax.rem(me + shift, n)}, device_id_type=MESH
        )

    def send_picks(distance):
        plane = lax.rem(my_plane + distance, planes)

        @pl.loop(0, PLANE)
        def _(turn):
            target = peer(plane, turn)

            @pl.when(target != me)
            def _():
                pltpu.make_async_remote_copy(
                    src_ref=chosen.at[target],
                    dst_ref=slots_s.at[me],
                    send_sem=pick_send,
                    recv_sem=pick_recv.at[my_plane],
                    device_id={"dp": target},
                    device_id_type=MESH,
                ).start()

    own_picks.wait()
    owner = lax.broadcasted_iota(jnp.int32, (n, capacity), 0)
    lane = lax.broadcasted_iota(jnp.int32, (n, capacity), 1)
    slot_lane = lax.broadcasted_iota(jnp.int32, (n, LANE), 1)
    local = picks[...] - owner * tok_dev
    before = jnp.sum((local < 0).astype(jnp.int32), axis=1, keepdims=True)
    place = lane - before
    label = jnp.where((local >= 0) & (local < tok_dev), local + 1, 0)
    table = jnp.full((n, LANE), tok_dev, jnp.int32)
    for slot in range(MOST):
        found = jnp.sum(jnp.where(place == slot, label, 0), axis=1, keepdims=True)
        table = jnp.where(slot_lane == slot, jnp.where(found > 0, found - 1, tok_dev), table)
    chosen[...] = table.reshape(n, 1, LANE)

    pl.semaphore_wait(barrier, n - 1)
    own_slots = pltpu.make_async_copy(chosen.at[me], slots_s.at[me], local_sem.at[2])
    own_slots.start()

    @pl.loop(0, planes)
    def _(turn):
        up, down = step_planes(GOING, turn // 2)
        send_picks(jnp.where(turn % 2 == 0, up, down) - my_plane + planes)


    matrix = swap_matrix()
    loads[0].wait()
    @pl.loop(0, tok_dev // (2 * SUB))
    def _(block):
        at = pl.multiple_of(block * 2 * SUB, 2 * SUB)
        tiles = to_tiles(matrix, tokens, at)
        for index, tile in enumerate(tiles):
            token_tiles[at + index] = tile

    token_tiles[tok_dev] = jnp.zeros((SUB, LANE), jnp.bfloat16)
    for load in loads[2:]:
        load.start()

    def row_copy(target):
        return pltpu.make_async_remote_copy(
            src_ref=send_buf.at[target],
            dst_ref=recv_buf.at[me],
            send_sem=row_send,
            recv_sem=row_recv.at[my_plane],
            device_id={"dp": target},
            device_id_type=MESH,
        )

    def result_copy(target):
        return pltpu.make_async_remote_copy(
            src_ref=result_buf.at[target],
            dst_ref=return_buf.at[me],
            send_sem=result_send,
            recv_sem=result_recv.at[my_plane],
            device_id={"dp": target},
            device_id_type=MESH,
        )

    own_rows = pltpu.make_async_copy(send_buf.at[me], recv_buf.at[me], local_sem.at[0])
    own_results = pltpu.make_async_copy(result_buf.at[me], return_buf.at[me], local_sem.at[1])

    def send_plane(plane, copy, own, turned):
        @pl.loop(0, PLANE)
        def _(turn):
            target = peer(plane, turn) if turned else plane * PLANE + (turn // 2 + jnp.where(turn >= 6, -1, jnp.where(turn >= 4, 1, 0))) * 2 + turn % 2

            @pl.when(target != me)
            def _():
                copy(target).start()

            @pl.when(target == me)
            def _():
                own.start()

    def wait_plane(plane, buffer, semaphores, own):
        @pl.when(plane != my_plane)
        def _():
            part = buffer.at[pl.ds(plane * PLANE, PLANE)]
            pltpu.make_async_copy(part, part, semaphores.at[plane]).wait()

        @pl.when(plane == my_plane)
        def _():
            part = buffer.at[pl.ds(plane * PLANE, PLANE - 1)]
            pltpu.make_async_copy(part, part, semaphores.at[plane]).wait()
            if own is not None:
                own.wait()

    token_lane = lax.broadcasted_iota(jnp.int32, (PLANE, tok_dev), 1)

    def serve(plane):
        wait_plane(plane, slots_s, pick_recv, own_slots)

        @pl.loop(0, PLANE)
        def _(member):
            for slot in range(MOST):
                token = jnp.clip(slots_s[plane * PLANE + member, 0, slot], 0, tok_dev)
                send_buf[plane * PLANE + member, slot] = token_tiles[token]

        send_plane(plane, row_copy, own_rows, True)

    @pl.loop(0, 2 * steps)
    def _(turn):
        step = turn // 2

        up, down = step_planes(GOING, step)
        serve(jnp.where(turn % 2 == 0, up, down))

    slots_copy = pltpu.make_async_copy(slots_s, slots_v, slot_sem)
    slots_copy.start()
    loads[1].wait()
    logits = lax.dot_general(
        router[...], tokens[...], (((1,), (1,)), ((), ())), preferred_element_type=jnp.float32
    )
    powers = jnp.exp(logits - jnp.max(logits, axis=0, keepdims=True))
    shares = powers / jnp.sum(powers, axis=0, keepdims=True)
    gates_t[...] = (n * shares).astype(jnp.bfloat16).astype(jnp.float32)

    slots_copy.wait()

    @pl.loop(0, planes)
    def _(plane):
        gates = gates_t[pl.ds(pl.multiple_of(plane * PLANE, PLANE), PLANE), :]
        table = slots_v[pl.ds(plane * PLANE, PLANE)].reshape(PLANE, LANE)
        for slot in range(MOST):
            at = pl.multiple_of(plane * half + slot * PLANE, PLANE)
            mix_t[pl.ds(at, PLANE), :] = jnp.where(
                token_lane == table[:, slot : slot + 1], gates, 0.0
            )

    mix[...] = mix_t[...].T.astype(jnp.bfloat16)

    for load in loads[2:]:
        load.wait()

    @pl.loop(0, steps)
    def _(step):
        pair = step_planes(COMING, step)
        for plane in pair:
            wait_plane(plane, recv_buf, row_recv, own_rows)
        to_rows(matrix, recv_buf, pair, rows, 0)
        taken = rows[...]
        block = 256
        for at in range(0, gate_w.shape[1], block):
            gate_act = jnp.dot(taken, gate_w[:, at : at + block], preferred_element_type=jnp.float32)
            up_act = jnp.dot(taken, up_w[:, at : at + block], preferred_element_type=jnp.float32)
            hidden[:, at : at + block] = (
                gate_act / (1.0 + jnp.exp(-gate_act)) * up_act
            ).astype(jnp.bfloat16)
        held = hidden[...]
        for at in range(0, width, block):
            result_rows[:, at : at + block] = jnp.dot(
                held, down_w[:, at : at + block], preferred_element_type=jnp.float32
            ).astype(jnp.bfloat16)
        for pack in range(2 * half // (2 * SUB)):
            tiles = to_tiles(matrix, result_rows, pack * 2 * SUB)
            for index, tile in enumerate(tiles):
                row = pack * 2 * SUB + index
                plane = pair[row // half]
                slot, member = divmod(row % half, PLANE)
                result_buf[plane * PLANE + member, slot] = tile
        for plane in pair:
            send_plane(plane, result_copy, own_results, False)

    @pl.loop(0, steps)
    def _(step):
        for plane in step_planes(COMING, step):
            wait_plane(plane, return_buf, result_recv, own_results)
            to_rows(
                matrix, return_buf, (plane,), return_rows, pl.multiple_of(plane * half, SUB)
            )

    def drain(buffer, semaphore):
        part = buffer.at[pl.ds(0, n - 1)]
        pltpu.make_async_copy(part, part, semaphore).wait()

    drain(chosen, pick_send)
    drain(send_buf, row_send)
    drain(result_buf, result_send)


def add_up(weights_ref, returned, out_hbm, held, semaphores):
    weights = weights_ref[...]
    copies = []
    for at in range(0, held.shape[1], BLOCK):
        columns = pl.ds(at, BLOCK)
        held[:, columns] = jnp.dot(
            weights, returned[:, columns], preferred_element_type=jnp.float32
        ).astype(jnp.bfloat16)
        copies.append(
            pltpu.make_async_copy(
                held.at[:, columns], out_hbm.at[:, columns], semaphores.at[at // BLOCK]
            )
        )
        copies[-1].start()
    for copy in copies:
        copy.wait()


def layer(n, tokens, router, w_gate, w_up, w_down, picks):
    tok_dev, width = tokens.shape
    hidden_width = w_gate.shape[2]
    capacity = picks.shape[1]
    planes = n // PLANE
    vmem = pl.BlockSpec(memory_space=pltpu.VMEM)
    anywhere = pl.BlockSpec(memory_space=pl.ANY)
    block = (n, MOST, SUB, LANE)
    bf16 = jnp.bfloat16
    group = 2 * PLANE * MOST
    returned, weights = pl.pallas_call(
        functools.partial(kernel, n),
        out_shape=(
            jax.ShapeDtypeStruct((n * MOST, width), bf16),
            jax.ShapeDtypeStruct((tok_dev, n * MOST), bf16),
        ),
        in_specs=[anywhere] * 6,
        out_specs=(vmem, vmem),
        scratch_shapes=[
            pltpu.VMEM((tok_dev, width), bf16),
            pltpu.VMEM(router.shape[::-1], bf16),
            pltpu.VMEM((width, hidden_width), bf16),
            pltpu.VMEM((width, hidden_width), bf16),
            pltpu.VMEM((hidden_width, width), bf16),
            pltpu.VMEM((tok_dev + 1, SUB, LANE), bf16),
            pltpu.VMEM((n, tok_dev), jnp.float32),
            pltpu.VMEM((1, capacity), jnp.int32),
            pltpu.VMEM((n, 1, LANE), jnp.int32),
            pltpu.VMEM((n, 1, LANE), jnp.int32),
            pltpu.SMEM((n, 1, LANE), jnp.int32),
            pltpu.VMEM((n * MOST, tok_dev), jnp.float32),
            pltpu.VMEM(block, bf16),
            pltpu.VMEM(block, bf16),
            pltpu.VMEM((group, width), bf16),
            pltpu.VMEM((group, hidden_width), bf16),
            pltpu.VMEM((group, width), bf16),
            pltpu.VMEM(block, bf16),
            pltpu.VMEM(block, bf16),
            pltpu.SemaphoreType.DMA((5,)),
            pltpu.SemaphoreType.DMA,
            pltpu.SemaphoreType.DMA((3,)),
            pltpu.SemaphoreType.DMA,
            pltpu.SemaphoreType.DMA((planes,)),
            pltpu.SemaphoreType.DMA,
            pltpu.SemaphoreType.DMA((planes,)),
            pltpu.SemaphoreType.DMA,
            pltpu.SemaphoreType.DMA((planes,)),
        ],
        compiler_params=pltpu.CompilerParams(
            collective_id=0, has_side_effects=True, vmem_limit_bytes=32 * 2**20
        ),
    )(
        *[
            pltpu.with_memory_space_constraint(operand, pltpu.HBM)
            for operand in (tokens, router.T, w_gate, w_up, w_down, picks)
        ]
    )
    return pl.pallas_call(
        add_up,
        out_shape=jax.ShapeDtypeStruct((tok_dev, width), bf16),
        in_specs=[vmem, vmem],
        out_specs=pl.BlockSpec(memory_space=pltpu.HBM),
        scratch_shapes=[
            pltpu.VMEM((tok_dev, width), bf16),
            pltpu.SemaphoreType.DMA((width // BLOCK,)),
        ],
        compiler_params=pltpu.CompilerParams(vmem_limit_bytes=8 * 2**20),
    )(weights, returned)


def solution(mesh):
    n = mesh.shape["dp"]
    return jax.shard_map(
        functools.partial(layer, n),
        mesh=mesh,
        in_specs=(
            P(("rep", "dp"), None),
            P("rep", None),
            P("dp", None, None),
            P("dp", None, None),
            P("dp", None, None),
            P(("rep", "dp"), None),
        ),
        out_specs=P(("rep", "dp"), None),
        check_vma=False,
    )
```

```python
import functools

import jax
import jax.numpy as jnp
from jax import lax
from jax.experimental import pallas as pl
from jax.experimental.pallas import tpu as pltpu
from jax.sharding import PartitionSpec as P

BLOCK = 256
MOST = 6
PLANE = 8
SUB, LANE = 16, 128
MESH = pl.DeviceIdType.MESH
GOING = ((1, 7), (3, 5), (4, 0), (2, 6))
COMING = ((1, 7), (3, 5), (4, 0), (2, 6))


def swap_matrix():
    row = lax.broadcasted_iota(jnp.int32, (SUB * SUB, SUB * SUB), 0)
    col = lax.broadcasted_iota(jnp.int32, (SUB * SUB, SUB * SUB), 1)
    swapped = (col % SUB) * SUB + col // SUB
    return (row == swapped).astype(jnp.float32).astype(jnp.bfloat16)


def swap(matrix, stacked):
    return jnp.dot(matrix, stacked, preferred_element_type=jnp.float32).astype(jnp.bfloat16)


def plane_tiles(buffer, plane, part):
    tiles = [
        buffer[plane * PLANE + member, 2 * part + half]
        for half in range(2)
        for member in range(PLANE)
    ]
    return jnp.concatenate(tiles, axis=0)


def to_rows(matrix, buffer, planes, target, target_row):
    jobs = [(plane, part) for plane in planes for part in range(MOST // 2)]
    for first in range(0, len(jobs), 2):
        pair = jobs[first : first + 2]
        stacked = jnp.concatenate([plane_tiles(buffer, *job) for job in pair], axis=1)
        moved = swap(matrix, stacked)
        for which in range(len(pair)):
            at = target_row + (first + which) * SUB
            for chunk in range(SUB):
                target[pl.ds(at, SUB), chunk * LANE : (chunk + 1) * LANE] = moved[
                    chunk * SUB : (chunk + 1) * SUB, which * LANE : (which + 1) * LANE
                ]


def to_tiles(matrix, rows, first_row):
    def stack(at):
        return jnp.concatenate(
            [rows[pl.ds(at, SUB), chunk * LANE : (chunk + 1) * LANE] for chunk in range(SUB)],
            axis=0,
        )

    stacked = jnp.concatenate([stack(first_row), stack(first_row + SUB)], axis=1)
    moved = swap(matrix, stacked)
    return [
        moved[row * SUB : (row + 1) * SUB, half * LANE : (half + 1) * LANE]
        for half in range(2)
        for row in range(SUB)
    ]


def kernel(
    n,
    tokens_hbm,
    router_hbm,
    gate_hbm,
    up_hbm,
    down_hbm,
    picks_hbm,
    return_rows,
    mix,
    tokens,
    router,
    gate_w,
    up_w,
    down_w,
    token_tiles,
    gates_t,
    picks,
    chosen,
    slots_v,
    slots_s,
    mix_t,
    send_buf,
    recv_buf,
    rows,
    hidden,
    result_rows,
    result_buf,
    return_buf,
    load_sem,
    slot_sem,
    local_sem,
    pick_send,
    pick_recv,
    row_send,
    row_recv,
    result_send,
    result_recv,
):
    me = lax.axis_index("dp")
    planes = n // PLANE
    my_plane = me // PLANE
    tok_dev, width = tokens.shape
    capacity = picks.shape[1]
    steps = planes // 2
    my_member = lax.rem(me, PLANE)
    half = PLANE * MOST

    def peer(plane, turn):
        column = lax.rem(my_member // 2 + turn // 2, PLANE // 2)
        core = lax.rem(my_member + turn, 2)
        return plane * PLANE + column * 2 + core

    def step_planes(order, step):
        pair = order[-1]
        for index in range(steps - 1):
            pair = [jnp.where(step == index, *both) for both in zip(order[index], pair)]
        return [lax.rem(my_plane + distance, planes) for distance in pair]

    loads = [
        pltpu.make_async_copy(tokens_hbm, tokens, load_sem.at[0]),
        pltpu.make_async_copy(router_hbm, router, load_sem.at[1]),
        pltpu.make_async_copy(gate_hbm.at[0], gate_w, load_sem.at[2]),
        pltpu.make_async_copy(up_hbm.at[0], up_w, load_sem.at[3]),
        pltpu.make_async_copy(down_hbm.at[0], down_w, load_sem.at[4]),
    ]
    own_picks = pltpu.make_async_copy(picks_hbm, picks, local_sem.at[2])
    own_picks.start()
    for load in loads[:2]:
        load.start()

    barrier = pltpu.get_barrier_semaphore()

    @pl.loop(1, n)
    def _(shift):
        pl.semaphore_signal(
            barrier, inc=1, device_id={"dp": lax.rem(me + shift, n)}, device_id_type=MESH
        )

    def send_picks(distance):
        plane = lax.rem(my_plane + distance, planes)

        @pl.loop(0, PLANE)
        def _(turn):
            target = peer(plane, turn)

            @pl.when(target != me)
            def _():
                pltpu.make_async_remote_copy(
                    src_ref=chosen.at[target],
                    dst_ref=slots_s.at[me],
                    send_sem=pick_send,
                    recv_sem=pick_recv.at[my_plane],
                    device_id={"dp": target},
                    device_id_type=MESH,
                ).start()

    own_picks.wait()
    owner = lax.broadcasted_iota(jnp.int32, (n, capacity), 0)
    lane = lax.broadcasted_iota(jnp.int32, (n, capacity), 1)
    slot_lane = lax.broadcasted_iota(jnp.int32, (n, LANE), 1)
    local = picks[...] - owner * tok_dev
    before = jnp.sum((local < 0).astype(jnp.int32), axis=1, keepdims=True)
    place = lane - before
    label = jnp.where((local >= 0) & (local < tok_dev), local + 1, 0)
    table = jnp.full((n, LANE), tok_dev, jnp.int32)
    for slot in range(MOST):
        found = jnp.sum(jnp.where(place == slot, label, 0), axis=1, keepdims=True)
        table = jnp.where(slot_lane == slot, jnp.where(found > 0, found - 1, tok_dev), table)
    chosen[...] = table.reshape(n, 1, LANE)

    pl.semaphore_wait(barrier, n - 1)
    own_slots = pltpu.make_async_copy(chosen.at[me], slots_s.at[me], local_sem.at[2])
    own_slots.start()

    @pl.loop(0, planes)
    def _(turn):
        up, down = step_planes(GOING, turn // 2)
        send_picks(jnp.where(turn % 2 == 0, up, down) - my_plane + planes)


    matrix = swap_matrix()
    loads[0].wait()
    @pl.loop(0, tok_dev // (2 * SUB))
    def _(block):
        at = pl.multiple_of(block * 2 * SUB, 2 * SUB)
        tiles = to_tiles(matrix, tokens, at)
        for index, tile in enumerate(tiles):
            token_tiles[at + index] = tile

    token_tiles[tok_dev] = jnp.zeros((SUB, LANE), jnp.bfloat16)
    for load in loads[2:]:
        load.start()

    def row_copy(target):
        return pltpu.make_async_remote_copy(
            src_ref=send_buf.at[target],
            dst_ref=recv_buf.at[me],
            send_sem=row_send,
            recv_sem=row_recv.at[my_plane],
            device_id={"dp": target},
            device_id_type=MESH,
        )

    def result_copy(target):
        return pltpu.make_async_remote_copy(
            src_ref=result_buf.at[target],
            dst_ref=return_buf.at[me],
            send_sem=result_send,
            recv_sem=result_recv.at[my_plane],
            device_id={"dp": target},
            device_id_type=MESH,
        )

    own_rows = pltpu.make_async_copy(send_buf.at[me], recv_buf.at[me], local_sem.at[0])
    own_results = pltpu.make_async_copy(result_buf.at[me], return_buf.at[me], local_sem.at[1])

    def send_plane(plane, copy, own, turned):
        @pl.loop(0, PLANE)
        def _(turn):
            target = peer(plane, turn) if turned else plane * PLANE + (turn // 2 + jnp.where(turn >= 6, -1, jnp.where(turn >= 4, 1, 0))) * 2 + turn % 2

            @pl.when(target != me)
            def _():
                copy(target).start()

            @pl.when(target == me)
            def _():
                own.start()

    def wait_plane(plane, buffer, semaphores, own):
        @pl.when(plane != my_plane)
        def _():
            part = buffer.at[pl.ds(plane * PLANE, PLANE)]
            pltpu.make_async_copy(part, part, semaphores.at[plane]).wait()

        @pl.when(plane == my_plane)
        def _():
            part = buffer.at[pl.ds(plane * PLANE, PLANE - 1)]
            pltpu.make_async_copy(part, part, semaphores.at[plane]).wait()
            if own is not None:
                own.wait()

    token_lane = lax.broadcasted_iota(jnp.int32, (PLANE, tok_dev), 1)

    def serve(plane):
        wait_plane(plane, slots_s, pick_recv, own_slots)

        @pl.loop(0, PLANE)
        def _(member):
            for slot in range(MOST):
                token = jnp.clip(slots_s[plane * PLANE + member, 0, slot], 0, tok_dev)
                send_buf[plane * PLANE + member, slot] = token_tiles[token]

        send_plane(plane, row_copy, own_rows, True)

    @pl.loop(0, 2 * steps)
    def _(turn):
        step = turn // 2

        up, down = step_planes(GOING, step)
        serve(jnp.where(turn % 2 == 0, up, down))

    slots_copy = pltpu.make_async_copy(slots_s, slots_v, slot_sem)
    slots_copy.start()
    loads[1].wait()
    logits = lax.dot_general(
        router[...], tokens[...], (((1,), (1,)), ((), ())), preferred_element_type=jnp.float32
    )
    powers = jnp.exp(logits - jnp.max(logits, axis=0, keepdims=True))
    shares = powers / jnp.sum(powers, axis=0, keepdims=True)
    gates_t[...] = (n * shares).astype(jnp.bfloat16).astype(jnp.float32)

    slots_copy.wait()

    @pl.loop(0, planes)
    def _(plane):
        gates = gates_t[pl.ds(pl.multiple_of(plane * PLANE, PLANE), PLANE), :]
        table = slots_v[pl.ds(plane * PLANE, PLANE)].reshape(PLANE, LANE)
        for slot in range(MOST):
            at = pl.multiple_of(plane * half + slot * PLANE, PLANE)
            mix_t[pl.ds(at, PLANE), :] = jnp.where(
                token_lane == table[:, slot : slot + 1], gates, 0.0
            )

    mix[...] = mix_t[...].T.astype(jnp.bfloat16)

    for load in loads[2:]:
        load.wait()

    @pl.loop(0, steps)
    def _(step):
        pair = step_planes(COMING, step)
        for plane in pair:
            wait_plane(plane, recv_buf, row_recv, own_rows)
        to_rows(matrix, recv_buf, pair, rows, 0)
        taken = rows[...]
        block = 256
        for at in range(0, gate_w.shape[1], block):
            gate_act = jnp.dot(taken, gate_w[:, at : at + block], preferred_element_type=jnp.float32)
            up_act = jnp.dot(taken, up_w[:, at : at + block], preferred_element_type=jnp.float32)
            hidden[:, at : at + block] = (
                gate_act / (1.0 + jnp.exp(-gate_act)) * up_act
            ).astype(jnp.bfloat16)
        held = hidden[...]
        for at in range(0, width, block):
            result_rows[:, at : at + block] = jnp.dot(
                held, down_w[:, at : at + block], preferred_element_type=jnp.float32
            ).astype(jnp.bfloat16)
        for pack in range(2 * half // (2 * SUB)):
            tiles = to_tiles(matrix, result_rows, pack * 2 * SUB)
            for index, tile in enumerate(tiles):
                row = pack * 2 * SUB + index
                plane = pair[row // half]
                slot, member = divmod(row % half, PLANE)
                result_buf[plane * PLANE + member, slot] = tile
        for plane in pair:
            send_plane(plane, result_copy, own_results, False)

    @pl.loop(0, steps)
    def _(step):
        for plane in step_planes(COMING, step):
            wait_plane(plane, return_buf, result_recv, own_results)
            to_rows(
                matrix, return_buf, (plane,), return_rows, pl.multiple_of(plane * half, SUB)
            )

    def drain(buffer, semaphore):
        part = buffer.at[pl.ds(0, n - 1)]
        pltpu.make_async_copy(part, part, semaphore).wait()

    drain(chosen, pick_send)
    drain(send_buf, row_send)
    drain(result_buf, result_send)


def add_up(weights_ref, returned, out_hbm, held, semaphores):
    weights = weights_ref[...]
    copies = []
    for at in range(0, held.shape[1], BLOCK):
        columns = pl.ds(at, BLOCK)
        held[:, columns] = jnp.dot(
            weights, returned[:, columns], preferred_element_type=jnp.float32
        ).astype(jnp.bfloat16)
        copies.append(
            pltpu.make_async_copy(
                held.at[:, columns], out_hbm.at[:, columns], semaphores.at[at // BLOCK]
            )
        )
        copies[-1].start()
    for copy in copies:
        copy.wait()


def layer(n, tokens, router, w_gate, w_up, w_down, picks):
    tok_dev, width = tokens.shape
    hidden_width = w_gate.shape[2]
    capacity = picks.shape[1]
    planes = n // PLANE
    vmem = pl.BlockSpec(memory_space=pltpu.VMEM)
    anywhere = pl.BlockSpec(memory_space=pl.ANY)
    block = (n, MOST, SUB, LANE)
    bf16 = jnp.bfloat16
    group = 2 * PLANE * MOST
    returned, weights = pl.pallas_call(
        functools.partial(kernel, n),
        out_shape=(
            jax.ShapeDtypeStruct((n * MOST, width), bf16),
            jax.ShapeDtypeStruct((tok_dev, n * MOST), bf16),
        ),
        in_specs=[anywhere] * 6,
        out_specs=(vmem, vmem),
        scratch_shapes=[
            pltpu.VMEM((tok_dev, width), bf16),
            pltpu.VMEM(router.shape[::-1], bf16),
            pltpu.VMEM((width, hidden_width), bf16),
            pltpu.VMEM((width, hidden_width), bf16),
            pltpu.VMEM((hidden_width, width), bf16),
            pltpu.VMEM((tok_dev + 1, SUB, LANE), bf16),
            pltpu.VMEM((n, tok_dev), jnp.float32),
            pltpu.VMEM((1, capacity), jnp.int32),
            pltpu.VMEM((n, 1, LANE), jnp.int32),
            pltpu.VMEM((n, 1, LANE), jnp.int32),
            pltpu.SMEM((n, 1, LANE), jnp.int32),
            pltpu.VMEM((n * MOST, tok_dev), jnp.float32),
            pltpu.VMEM(block, bf16),
            pltpu.VMEM(block, bf16),
            pltpu.VMEM((group, width), bf16),
            pltpu.VMEM((group, hidden_width), bf16),
            pltpu.VMEM((group, width), bf16),
            pltpu.VMEM(block, bf16),
            pltpu.VMEM(block, bf16),
            pltpu.SemaphoreType.DMA((5,)),
            pltpu.SemaphoreType.DMA,
            pltpu.SemaphoreType.DMA((3,)),
            pltpu.SemaphoreType.DMA,
            pltpu.SemaphoreType.DMA((planes,)),
            pltpu.SemaphoreType.DMA,
            pltpu.SemaphoreType.DMA((planes,)),
            pltpu.SemaphoreType.DMA,
            pltpu.SemaphoreType.DMA((planes,)),
        ],
        compiler_params=pltpu.CompilerParams(
            collective_id=0, has_side_effects=True, vmem_limit_bytes=32 * 2**20
        ),
    )(
        *[
            pltpu.with_memory_space_constraint(operand, pltpu.HBM)
            for operand in (tokens, router.T, w_gate, w_up, w_down, picks)
        ]
    )
    return pl.pallas_call(
        add_up,
        out_shape=jax.ShapeDtypeStruct((tok_dev, width), bf16),
        in_specs=[vmem, vmem],
        out_specs=pl.BlockSpec(memory_space=pltpu.HBM),
        scratch_shapes=[
            pltpu.VMEM((tok_dev, width), bf16),
            pltpu.SemaphoreType.DMA((width // BLOCK,)),
        ],
        compiler_params=pltpu.CompilerParams(vmem_limit_bytes=8 * 2**20),
    )(weights, returned)


def solution(mesh):
    n = mesh.shape["dp"]
    return jax.shard_map(
        functools.partial(layer, n),
        mesh=mesh,
        in_specs=(
            P(("rep", "dp"), None),
            P("rep", None),
            P("dp", None, None),
            P("dp", None, None),
            P("dp", None, None),
            P(("rep", "dp"), None),
        ),
        out_specs=P(("rep", "dp"), None),
        check_vma=False,
    )
```
